32 devices in a mesh: dp: 16 (over z, y, x), width: 2 (over core).
Axes of the slice: x: 2, y: 2, z: 4, core: 2. Of those that a mesh axis runs over, the one named last changes fastest.
Arguments:
- train_act: bfloat16 [4096, 28672], P('dp', 'width'), may hold values from -6 to 6
- train_grad: bfloat16 [4096, 8192], P('dp', 'width'), may hold values from -6 to 6
- val_act: bfloat16 [512, 28672], P('dp', 'width'), may hold values from -6 to 6
- val_grad: bfloat16 [512, 8192], P('dp', 'width'), may hold values from -6 to 6
Outputs:
- token_scores: float32 [2, 4096], P(None, 'dp')
The draws below stay inside these ranges and needn't reach their ends.
All inputs are finite; a program needn't handle non-finite values.
Results may differ from the reference program's by a relative error of at most 0.0003.
Values may be sent and summed in bfloat16 or wider, within the bound.
No kernel may reach another device: no remote copies, remote signals or barrier semaphores. Data moves between devices by JAX's collectives and lax.ppermute only.
A program may use at most 128 MiB of HBM per device.

```python
import jax
import jax.numpy as jnp

D = 8192
FF = 28672
VSEQ = 2
VLEN = 256
VTOK = 512
TOKENS = 4096


def block_levels(rng, dims, pieces, smallest, high):
    gain = 1.0
    for position, blocks in pieces:
        heights = jax.random.uniform(jax.random.fold_in(jax.random.fold_in(rng, 6), position), (blocks,), jnp.float32, smallest / len(pieces), high / len(pieces))
        gain = gain * jnp.repeat(jnp.exp(heights), dims[position] // blocks).reshape((-1,) + (1,) * (len(dims) - 1 - position))
    return gain


def bell_draw(stream_key, shape, spread, most, cuts=(), held_as=jnp.bfloat16):
    entries = jax.random.normal(stream_key, shape, jnp.float32) * spread
    if len(cuts) > 0:
        entries = block_levels(stream_key, shape, cuts, -0.22, 0.18) * entries
    return jnp.clip(entries, min=-most, max=most).astype(held_as)


def setup_inputs(seed: int = 0) -> dict:
    streams_of = jax.random.split(jax.random.key(seed), 5)
    train_act = bell_draw(streams_of[0], (TOKENS, FF), 1.0, 6.0, ((0, 16), (1, 2)))
    train_grad = bell_draw(streams_of[1], (TOKENS, D), 1.0, 6.0, ((0, 16), (1, 2)))
    val_act = bell_draw(streams_of[2], (VTOK, FF), 1.0, 6.0, ((0, 16), (1, 2)))
    val_grad = bell_draw(streams_of[3], (VTOK, D), 1.0, 6.0, ((0, 16), (1, 2)))
    return dict(train_act=train_act, train_grad=train_grad, val_act=val_act, val_grad=val_grad)


def reference(train_act, train_grad, val_act, val_grad):
    act_gram = jnp.dot(train_act, val_act.T, preferred_element_type=jnp.float32)
    grad_gram = jnp.dot(train_grad, val_grad.T, preferred_element_type=jnp.float32)
    product = act_gram * grad_gram
    summed = product.reshape(product.shape[0], VSEQ, VLEN).sum(axis=-1)
    scale = 1.0 / jnp.sqrt(jnp.float32(FF) * jnp.float32(D) * jnp.float32(VLEN))
    return (summed * scale).T
```

```python
import jax
import jax.numpy as jnp
from jax import lax
from jax.sharding import PartitionSpec as P


D = 8192
FF = 28672
VLEN = 256


def outer_rows(left, right):
    return lax.dot_general(
        left, right, (((1,), (1,)), ((), ())), preferred_element_type=jnp.float32
    )


def scale_of():
    return 1.0 / jnp.sqrt(jnp.float32(FF) * jnp.float32(D) * jnp.float32(VLEN))


def gathered(train_act, train_grad, val_act, val_grad):
    gram = 1.0
    for train, val in ((train_act, val_act), (train_grad, val_grad)):
        whole = lax.all_gather(val, "dp", axis=0, tiled=True)
        gram = gram * lax.psum(outer_rows(train, whole), "width")
    return (gram.reshape(gram.shape[0], -1, VLEN).sum(axis=-1) * scale_of()).T


def make_shards(dp, width):
    line, inner = 4, 16
    outer = dp // inner

    def pairs_of(step):
        pairs = []
        for o in range(outer):
            for z in range(line):
                for y in range(2):
                    for x in range(2):
                        to = step(z, y, x)
                        if to is not None:
                            source = ((o * line + z) * 2 + y) * 2 + x
                            pairs.append((source, ((o * line + to[0]) * 2 + to[1]) * 2 + to[2]))
        return pairs

    over_x = pairs_of(lambda z, y, x: (z, y, 1 - x))
    over_y = pairs_of(lambda z, y, x: (z, 1 - y, x))
    outside = pairs_of(lambda z, y, x: (z ^ 1, y, x))
    middle = pairs_of(lambda z, y, x: (3 - z if z in (1, 2) else z, y, x))

    def move(value, pairs, axis="dp"):
        return lax.ppermute(value, axis, pairs)

    def halves(array, place):
        half = array.shape[1] // 2
        first, second = array[:, :half], array[:, half:]
        return jnp.where(place == 0, first, second), jnp.where(place == 0, second, first)

    def in_order(place, mine, theirs):
        first = jnp.where(place == 0, mine, theirs)
        second = jnp.where(place == 0, theirs, mine)
        return first, second

    def along(value, is_middle):
        near = move(value, outside)
        across = move(value, middle)
        beyond = move(near, middle)
        third = jnp.where(is_middle, across, move(across, outside))
        fourth = jnp.where(is_middle, beyond, move(beyond, outside))
        return near, third, fourth

    def shards(train_act, train_grad, val_act, val_grad):
        return body(train_act, train_grad, val_act, val_grad)

    def body(train_act, train_grad, val_act, val_grad):
        me = lax.axis_index("dp")
        x, y, z = me % 2, (me // 2) % 2, (me // 4) % line
        is_middle = (z == 1) | (z == 2)
        if outer > 1:
            groups = [[o * inner + i for o in range(outer)] for i in range(inner)]
            val_act, val_grad = (
                lax.all_gather(v, "dp", axis=0, tiled=True, axis_index_groups=groups)
                for v in (val_act, val_grad)
            )
        rows = val_act.shape[0]

        act, act_out = halves(val_act, x)
        grad, grad_out = halves(val_grad, y)
        act = jnp.concatenate(in_order(x, act, move(act_out, over_x)), axis=0)
        grad_far = move(grad_out, over_y)
        grad = jnp.concatenate(in_order(y, grad, grad_far), axis=0).reshape(2, rows, -1)
        grad_far = move(grad, over_x)
        grad = jnp.concatenate(in_order(x, grad, grad_far), axis=1).reshape(4 * rows, -1)
        own_act, out_act = halves(train_act, x)
        own_grad, out_grad = halves(train_grad, y)
        far_act = move(out_act, over_x)
        far_grad = move(out_grad, over_y)

        acts = (act,) + along(act, is_middle)
        grads = (grad,) + along(grad, is_middle)
        others = [move(a, over_y) for a in acts]

        mine = jnp.concatenate(acts, axis=0)
        theirs, pairs = [], []
        for i in range(2):
            theirs.append(jnp.concatenate(others[2 * i : 2 * i + 2], axis=0))
            pairs.append(jnp.concatenate(
                [g[h * 2 * rows : (h + 1) * 2 * rows] for h in range(2) for g in grads[2 * i : 2 * i + 2]],
                axis=0,
            ))
        far = jnp.concatenate([outer_rows(far_act, mine), outer_rows(far_act, theirs[0])], axis=1)
        act_back = move(far, over_x)
        far = outer_rows(far_act, theirs[1])
        act_last = move(far, over_x)
        grad_own, grad_back = [], []
        for pair in pairs:
            far = outer_rows(far_grad, pair)
            grad_back.append(move(far, over_y))
            grad_own.append(outer_rows(own_grad, pair))
        act_mine, act_first = outer_rows(own_act, mine), outer_rows(own_act, theirs[0])
        act_second = outer_rows(own_act, theirs[1])
        act_mine, act_first, act_second = lax.optimization_barrier((act_mine, act_first, act_second))
        n = 4 * rows
        act_gram = jnp.concatenate([
            act_mine + act_back[:, : 2 * n],
            jnp.concatenate([act_first + act_back[:, 2 * n :], act_second + act_last], axis=1),
        ], axis=0)
        grad_gram = jnp.concatenate(grad_own, axis=1) + jnp.concatenate(grad_back, axis=1)
        if width == 2:
            act_gram = act_gram + move(act_gram, [(0, 1), (1, 0)], "width")
            grad_gram = grad_gram + move(grad_gram, [(0, 1), (1, 0)], "width")

        tokens = grad_gram.shape[0]
        one, two = in_order(y, act_gram[:tokens], act_gram[tokens:])
        local = rows // outer
        column = jnp.arange(2 * rows)
        plane = (z, z ^ 1, jnp.where(z < 2, 2, 1), jnp.where(z < 2, 3, 0))
        scores = [0.0] * (dp * local // VLEN)
        for i in range(2):
            for yy, gram in enumerate((one, two)):
                product = gram[:, i * n : (i + 1) * n] * grad_gram[:, (2 * i + yy) * n : (2 * i + yy + 1) * n]
                sequence = []
                for p in plane[2 * i : 2 * i + 2]:
                    device = (column % rows // local) * inner + p * 4 + yy * 2 + column // rows
                    sequence.append((device * local + column % local) // VLEN)
                sequence = jnp.concatenate(sequence)
                for v in range(len(scores)):
                    scores[v] = scores[v] + jnp.where(sequence == v, product, 0.0).sum(axis=1)
        return jnp.stack(scores) * scale_of()

    return shards


def solution(mesh):
    in_specs = (P("dp", "width"), P("dp", "width"), P("dp", "width"), P("dp", "width"))
    out_specs = P(None, "dp")
    dp, width = mesh.shape["dp"], mesh.shape["width"]
    if dp % 16 or width > 2:
        return jax.shard_map(gathered, mesh=mesh, in_specs=in_specs, out_specs=out_specs, check_vma=False)
    return jax.shard_map(
        make_shards(dp, width), mesh=mesh, in_specs=in_specs, out_specs=out_specs, check_vma=False
    )
```

```python
import jax
import jax.numpy as jnp
from jax import lax
from jax.sharding import PartitionSpec as P


D = 8192
FF = 28672
VLEN = 256


def outer_rows(left, right):
    return lax.dot_general(
        left, right, (((1,), (1,)), ((), ())), preferred_element_type=jnp.float32
    )


def scale_of():
    return 1.0 / jnp.sqrt(jnp.float32(FF) * jnp.float32(D) * jnp.float32(VLEN))


def gathered(train_act, train_grad, val_act, val_grad):
    gram = 1.0
    for train, val in ((train_act, val_act), (train_grad, val_grad)):
        whole = lax.all_gather(val, "dp", axis=0, tiled=True)
        gram = gram * lax.psum(outer_rows(train, whole), "width")
    return (gram.reshape(gram.shape[0], -1, VLEN).sum(axis=-1) * scale_of()).T


def make_shards(dp, width):
    line, inner = 4, 16
    outer = dp // inner

    def pairs_of(step):
        pairs = []
        for o in range(outer):
            for z in range(line):
                for y in range(2):
                    for x in range(2):
                        to = step(z, y, x)
                        if to is not None:
                            source = ((o * line + z) * 2 + y) * 2 + x
                            pairs.append((source, ((o * line + to[0]) * 2 + to[1]) * 2 + to[2]))
        return pairs

    over_x = pairs_of(lambda z, y, x: (z, y, 1 - x))
    over_y = pairs_of(lambda z, y, x: (z, 1 - y, x))
    outside = pairs_of(lambda z, y, x: (z ^ 1, y, x))
    middle = pairs_of(lambda z, y, x: (3 - z if z in (1, 2) else z, y, x))

    def move(value, pairs, axis="dp"):
        return lax.ppermute(value, axis, pairs)

    def halves(array, place):
        half = array.shape[1] // 2
        first, second = array[:, :half], array[:, half:]
        return jnp.where(place == 0, first, second), jnp.where(place == 0, second, first)

    def in_order(place, mine, theirs):
        first = jnp.where(place == 0, mine, theirs)
        second = jnp.where(place == 0, theirs, mine)
        return first, second

    def along(value, is_middle):
        near = move(value, outside)
        across = move(value, middle)
        beyond = move(near, middle)
        third = jnp.where(is_middle, across, move(across, outside))
        fourth = jnp.where(is_middle, beyond, move(beyond, outside))
        return near, third, fourth

    def shards(train_act, train_grad, val_act, val_grad):
        return body(train_act, train_grad, val_act, val_grad)

    def body(train_act, train_grad, val_act, val_grad):
        me = lax.axis_index("dp")
        x, y, z = me % 2, (me // 2) % 2, (me // 4) % line
        is_middle = (z == 1) | (z == 2)
        if outer > 1:
            groups = [[o * inner + i for o in range(outer)] for i in range(inner)]
            val_act, val_grad = (
                lax.all_gather(v, "dp", axis=0, tiled=True, axis_index_groups=groups)
                for v in (val_act, val_grad)
            )
        rows = val_act.shape[0]

        act, act_out = halves(val_act, x)
        grad, grad_out = halves(val_grad, y)
        act = jnp.concatenate(in_order(x, act, move(act_out, over_x)), axis=0)
        grad_far = move(grad_out, over_y)
        grad = jnp.concatenate(in_order(y, grad, grad_far), axis=0).reshape(2, rows, -1)
        grad_far = move(grad, over_x)
        grad = jnp.concatenate(in_order(x, grad, grad_far), axis=1).reshape(4 * rows, -1)
        own_act, out_act = halves(train_act, x)
        own_grad, out_grad = halves(train_grad, y)
        far_act = move(out_act, over_x)
        far_grad = move(out_grad, over_y)

        acts = (act,) + along(act, is_middle)
        grads = (grad,) + along(grad, is_middle)
        others = [move(a, over_y) for a in acts]

        mine = jnp.concatenate(acts, axis=0)
        theirs = jnp.concatenate(others[:3], axis=0)
        far = jnp.concatenate([outer_rows(mine, far_act), outer_rows(theirs, far_act)], axis=0)
        grad_far = jnp.concatenate([outer_rows(g, far_grad) for g in grads[:3]], axis=0)
        act_back = move(far, over_x)
        if width == 2:
            core = lax.axis_index("width")
            top, bottom = jnp.split(grad_far, 2, axis=0)
            keep, give = in_order(core, top, bottom)
            grad_back = move(keep + move(give, [(0, 1), (1, 0)], "width"), over_y)
            grad_back = jnp.concatenate(in_order(core, grad_back, jnp.zeros_like(grad_back)), axis=0)
        else:
            grad_back = move(grad_far, over_y)
        grad_far = outer_rows(grads[3], far_grad)
        grad_last = move(grad_far, over_y)
        far = outer_rows(others[3], far_act)
        act_last = move(far, over_x)
        grad_own = [outer_rows(g, own_grad) for g in grads[:2]]
        grad_own += [outer_rows(g, own_grad) for g in grads[2:]]
        act_own = [outer_rows(mine, own_act), outer_rows(theirs, own_act)]
        act_own.append(outer_rows(others[3], own_act))
        act_own = jnp.concatenate(lax.optimization_barrier(tuple(act_own)), axis=0)
        act_gram = act_own + jnp.concatenate([act_back, act_last], axis=0)
        grad_gram = jnp.concatenate(grad_own, axis=0) + jnp.concatenate([grad_back, grad_last], axis=0)
        if width == 2:
            act_gram = act_gram + move(act_gram, [(0, 1), (1, 0)], "width")
            grad_gram = grad_gram + move(grad_gram, [(0, 1), (1, 0)], "width")

        h = 2 * rows
        local = rows // outer
        row = jnp.arange(h)[:, None]
        one, two = in_order(y, act_gram[: 4 * h], act_gram[4 * h :])
        scores = [0.0] * (dp * local // VLEN)
        for slot, plane in enumerate((z, z ^ 1, jnp.where(z < 2, 2, 1), jnp.where(z < 2, 3, 0))):
            for yy, gram in enumerate((one, two)):
                product = gram[slot * h : (slot + 1) * h] * grad_gram[(2 * slot + yy) * h : (2 * slot + yy + 1) * h]
                device = (row % rows // local) * inner + plane * 4 + yy * 2 + row // rows
                sequence = (device * local + row % local) // VLEN
                for v in range(len(scores)):
                    scores[v] = scores[v] + jnp.where(sequence == v, product, 0.0).sum(axis=0)
        return jnp.stack(scores) * scale_of()

    return shards


def solution(mesh):
    in_specs = (P("dp", "width"), P("dp", "width"), P("dp", "width"), P("dp", "width"))
    out_specs = P(None, "dp")
    dp, width = mesh.shape["dp"], mesh.shape["width"]
    if dp % 16 or width > 2:
        return jax.shard_map(gathered, mesh=mesh, in_specs=in_specs, out_specs=out_specs, check_vma=False)
    return jax.shard_map(
        make_shards(dp, width), mesh=mesh, in_specs=in_specs, out_specs=out_specs, check_vma=False
    )
```
